32 devices in a mesh: tp: 4 (over z), dp: 8 (over y, x, core).
Axes of the slice: x: 2, y: 2, z: 4, core: 2. Of those that a mesh axis runs over, the one named last changes fastest.
Arguments:
- hidden: bfloat16 [8, 1024, 2048], P('dp')
- residual: float32 [8, 1024, 2048], P('dp')
- targets: int32 [8, 1024], P('dp')
- embedding: bfloat16 [50288, 2048], P('tp')
- norm_w: float32 [2048], replicated
Outputs:
- output 1: float32 [], replicated
- output 2: float32 [8, 1024, 2048], P('dp')
- output 3: float32 [50288, 2048], P('tp')
- output 4: float32 [2048], replicated
All inputs are finite; a program needn't handle non-finite values.
Results may differ from the reference program's by a relative error of at most 0.001.
Values sent between devices are 32-bit elements.
A program may use at most 1 GiB of HBM per device.

```python
import jax
import jax.numpy as jnp
from jax import lax

BATCH = 8
SEQ = 1024
D = 2048
VOCAB = 50288
NORM_EPS = 1e-5
HEAD_SCALE = 2.0
TOK_BLOCK = min(SEQ, 256)


def draw_targets(tgt_key):
    k_pick, k_head, k_wide = jax.random.split(tgt_key, 3)
    pick_wide = jax.random.randint(k_pick, (BATCH, SEQ), 0, 4)
    head_ids = jax.random.randint(k_head, (BATCH, SEQ), 0, VOCAB // 16)
    wide_ids = jax.random.randint(k_wide, (BATCH, SEQ), 0, VOCAB)
    targets = jnp.where(pick_wide == 0, wide_ids, head_ids)
    return targets.at[0, 0].set(VOCAB - 1).at[0, 1].set(0).astype(jnp.int32)


def setup_inputs(seed: int = 0) -> dict:
    root_key = jax.random.key(seed)
    k_hid, k_res, k_tgt, k_emb, k_norm = jax.random.split(root_key, 5)
    hidden = jax.random.normal(k_hid, (BATCH, SEQ, D), jnp.float32).astype(jnp.bfloat16)
    residual = jax.random.normal(k_res, (BATCH, SEQ, D), jnp.float32)
    targets = draw_targets(k_tgt)
    embedding = (jax.random.normal(k_emb, (VOCAB, D), jnp.float32) * (HEAD_SCALE * D ** -0.5)).astype(jnp.bfloat16)
    norm_w = 1.0 + 0.3 * jax.random.normal(k_norm, (D,), jnp.float32)
    return {'hidden': hidden, 'residual': residual, 'targets': targets, 'embedding': embedding, 'norm_w': norm_w}


def norm_apply(resid, norm_w):
    inv_rms = lax.rsqrt(jnp.mean(resid * resid, axis=-1, keepdims=True) + NORM_EPS)
    return resid * inv_rms * norm_w


def reference(hidden, residual, targets, embedding, norm_w):
    n_tok = BATCH * SEQ
    inv_n = 1.0 / n_tok
    n_blocks = n_tok // TOK_BLOCK
    resid_all = (residual + hidden.astype(jnp.float32)).reshape(n_blocks, TOK_BLOCK, D)
    tgt_all = targets.reshape(n_blocks, TOK_BLOCK)
    vocab_ids = jnp.arange(VOCAB, dtype=jnp.int32)

    def block_step(carry_acc, blk_inputs):
        grad_emb, grad_w, loss_sum = carry_acc
        resid_blk, tgt_blk = blk_inputs
        normed, norm_vjp = jax.vjp(norm_apply, resid_blk, norm_w)
        h_blk = normed.astype(jnp.bfloat16)
        logits = jnp.dot(h_blk, embedding.T, preferred_element_type=jnp.float32)
        row_max = jnp.max(logits, axis=-1, keepdims=True)
        exp_shift = jnp.exp(logits - row_max)
        sum_exp = jnp.sum(exp_shift, axis=-1, keepdims=True)
        is_target = vocab_ids[None, :] == tgt_blk[:, None]
        tgt_logit = jnp.sum(jnp.where(is_target, logits, 0.0), axis=-1)
        log_norm = row_max[:, 0] + jnp.log(sum_exp[:, 0])
        prob_rows = exp_shift / sum_exp
        dlogits = (jnp.where(is_target, prob_rows - 1.0, prob_rows) * inv_n).astype(jnp.bfloat16)
        grad_h = jnp.dot(dlogits, embedding, preferred_element_type=jnp.float32)
        grad_r, grad_wb = norm_vjp(grad_h)
        grad_emb = grad_emb + jnp.dot(dlogits.T, h_blk, preferred_element_type=jnp.float32)
        return (grad_emb, grad_w + grad_wb, loss_sum + jnp.sum(log_norm - tgt_logit)), grad_r

    init_acc = (jnp.zeros((VOCAB, D), jnp.float32), jnp.zeros((D,), jnp.float32), jnp.zeros((), jnp.float32))
    final_acc, grad_rows = lax.scan(block_step, init_acc, (resid_all, tgt_all))
    grad_emb, grad_w, loss_sum = final_acc
    return (loss_sum * inv_n, grad_rows.reshape(BATCH, SEQ, D), grad_emb, grad_w)
```

```python
import functools

import jax
import jax.numpy as jnp
from jax import lax
from jax.experimental import pallas as pl
from jax.experimental.pallas import tpu as pltpu
from jax.sharding import PartitionSpec as P


EPS = 1e-5
NEG = -3.0e38
VMEM_CAP = 66 * 1024 * 1024
NT = (((1,), (1,)), ((), ()))
NN = (((1,), (0,)), ((), ()))
TN = (((0,), (0,)), ((), ()))
VB = 1280
SUB = 256
TB = 128
R = 704
NF = 5
GROUPS = (2, 2, 1)


def params(**kw):
    return pltpu.CompilerParams(vmem_limit_bytes=VMEM_CAP, **kw)


def cost(flops, nbytes, exps=0):
    return pl.CostEstimate(flops=int(flops), bytes_accessed=int(nbytes), transcendentals=int(exps))


def whole(shape):
    return pl.BlockSpec(shape, lambda *a: (0,) * len(shape), pipeline_mode=pl.Buffered(1))


def norm_body(hid_ref, res_ref, w_ref, *refs):
    hb_ref, inv_ref, hf_ref = refs[-3:]
    r = res_ref[...] + hid_ref[...].astype(jnp.float32)
    inv = lax.rsqrt(jnp.mean(r * r, axis=-1, keepdims=True) + EPS)
    h = (r * inv * w_ref[...]).astype(jnp.bfloat16)
    hb_ref[...] = h
    hf_ref[...] = h.astype(jnp.float32)
    inv_ref[...] = inv


def norm_fwd(hid, res, w, half, so_far=()):
    n, d = hid.shape
    steps = n // (2 * TB)
    src = pl.BlockSpec((TB, d), lambda i: (i + half * steps, 0))
    return pl.pallas_call(
        norm_body, grid=(steps,),
        out_shape=(jax.ShapeDtypeStruct((n, d), jnp.bfloat16), jax.ShapeDtypeStruct((n, 1), jnp.float32),
                   jax.ShapeDtypeStruct((n // 2, d), jnp.float32)),
        in_specs=[src, src, whole((1, d))] + [pl.BlockSpec(memory_space=pl.ANY)] * len(so_far),
        out_specs=[src, pl.BlockSpec((TB, 1), lambda i: (i + half * steps, 0)), pl.BlockSpec((TB, d), lambda i: (i, 0))],
        input_output_aliases={3: 0, 4: 1} if so_far else {},
        cost_estimate=cost(8 * n * d, 6 * n * d), compiler_params=params(), name="norm_fwd")(hid, res, w, *so_far)


def fwd_body(vocab, h_ref, e_ref, lg_ref, st_ref, m_scr, s_scr):
    i = pl.program_id(0)
    n = h_ref.shape[0]

    @pl.when(i == 0)
    def _():
        m_scr[...] = jnp.full_like(m_scr, NEG)
        s_scr[...] = jnp.zeros_like(s_scr)

    def dot(k):
        return lax.dot_general(e_ref[pl.ds(k * SUB, SUB), :], h_ref[...], NT, preferred_element_type=jnp.float32)

    def stats(l, k):
        if (k + 1) * SUB > vocab % VB:
            row = lax.broadcasted_iota(jnp.int32, (SUB, 1), 0)
            l = jnp.where(row < vocab - i * VB - k * SUB, l, NEG)
        lg_ref[pl.ds(k * SUB, SUB), :] = l
        m_old = m_scr[...]
        l = l.reshape(SUB // 8, 8, n)
        m_new = jnp.maximum(m_old, jnp.max(l, axis=0))
        m_scr[...] = m_new
        s_scr[...] = s_scr[...] * jnp.exp(m_old - m_new) + jnp.sum(jnp.exp(l - m_new[None]), axis=0)

    l = dot(0)
    for k in range(VB // SUB):
        after = dot(k + 1) if (k + 1) * SUB < VB else None
        stats(l, k)
        l = after

    @pl.when(i == pl.num_programs(0) - 1)
    def _():
        m = m_scr[...]
        mx = jnp.max(m, axis=0, keepdims=True)
        sm = jnp.sum(s_scr[...] * jnp.exp(m - mx), axis=0, keepdims=True)
        row = lax.broadcasted_iota(jnp.int32, (8, 1), 0)
        st_ref[...] = jnp.where(row == 0, mx, sm)


def forward(h, emb):
    n, d = h.shape
    vocab = emb.shape[0]
    nb = pl.cdiv(vocab, VB)
    return pl.pallas_call(
        functools.partial(fwd_body, vocab), grid=(nb,),
        out_shape=(jax.ShapeDtypeStruct((nb * VB, n), jnp.float32), jax.ShapeDtypeStruct((8, n), jnp.float32)),
        in_specs=[whole((n, d)), pl.BlockSpec((VB, d), lambda i: (i, 0))],
        out_specs=[pl.BlockSpec((VB, n), lambda i: (i, 0)), pl.BlockSpec((8, n), lambda i: (0, 0))],
        scratch_shapes=[pltpu.VMEM((8, n), jnp.float32)] * 2,
        cost_estimate=cost(2 * n * d * vocab, 2 * vocab * d + 4 * n * vocab, n * vocab),
        compiler_params=params(), name="forward")(h, emb)


def dh_body(vocab, inv_n, lg_ref, e_ref, st_ref, inv_ref, hid_ref, res_ref, dh_ref, t_ref, hid_scr, res_scr, t_scr, sem):
    i = pl.program_id(0)
    n = st_ref.shape[1]
    loads = [pltpu.make_async_copy(hid_ref, hid_scr, sem.at[0]), pltpu.make_async_copy(res_ref, res_scr, sem.at[1])]

    @pl.when(i == 0)
    def _():
        for c in loads:
            c.start()
        dh_ref[...] = jnp.zeros_like(dh_ref)
        t_scr[...] = jnp.zeros_like(t_scr)

    m, si = st_ref[0:1], st_ref[1:2]
    row = lax.broadcasted_iota(jnp.int32, (SUB, 1), 0)
    rowf = row.astype(jnp.float32)

    def dlogits(k):
        l = lg_ref[pl.ds(k * SUB, SUB), :]
        p = jnp.exp(l - m) * si
        hit = rowf == st_ref[2:3] - (i * VB + k * SUB).astype(jnp.float32)
        t = t_scr[...]
        for u in range(SUB // 8):
            t = jnp.where(hit[u * 8:(u + 1) * 8], l[u * 8:(u + 1) * 8], t)
        t_scr[...] = t
        return jnp.where(hit, p - inv_n, p).astype(jnp.bfloat16)

    g = dlogits(0)
    for k in range(VB // SUB):
        after = dlogits(k + 1) if (k + 1) * SUB < VB else None
        e = e_ref[pl.ds(k * SUB, SUB), :]
        if (k + 1) * SUB > vocab % VB:
            e = jnp.where(row < vocab - i * VB - k * SUB, e, 0)
        dh_ref[pl.ds(0, n), :] += lax.dot_general(g, e, TN, preferred_element_type=jnp.float32)
        g = after

    @pl.when(i == pl.num_programs(0) - 1)
    def _():
        for c in loads:
            c.wait()
        t_ref[...] = t_scr[...]
        acc = jnp.zeros((8, dh_ref.shape[1]), jnp.float32)
        for q in range(n // TB):
            rows = pl.ds(q * TB, TB)
            v = dh_ref[rows, :] * ((res_scr[rows, :] + hid_scr[rows, :].astype(jnp.float32)) * inv_ref[rows, :])
            for u in range(TB // 8):
                acc = acc + v[u * 8:(u + 1) * 8]
        dh_ref[pl.ds(n, 8), :] = acc


def backward_h(lg, emb, st, inv, hid, res, inv_n):
    n, d = hid.shape
    vocab = emb.shape[0]
    any_space = pl.BlockSpec(memory_space=pl.ANY)
    return pl.pallas_call(
        functools.partial(dh_body, vocab, inv_n), grid=(lg.shape[0] // VB,),
        out_shape=(jax.ShapeDtypeStruct((n + 8, d), jnp.float32), jax.ShapeDtypeStruct((8, n), jnp.float32)),
        in_specs=[pl.BlockSpec((VB, n), lambda i: (i, 0)), pl.BlockSpec((VB, d), lambda i: (i, 0)), whole((8, n)), whole((n, 1)),
                  any_space, any_space],
        out_specs=[whole((n + 8, d)), pl.BlockSpec((8, n), lambda i: (0, 0))],
        scratch_shapes=[pltpu.VMEM((n, d), jnp.bfloat16), pltpu.VMEM((n, d), jnp.float32), pltpu.VMEM((8, n), jnp.float32),
                        pltpu.SemaphoreType.DMA((2,))],
        cost_estimate=cost(2 * n * d * vocab, 2 * vocab * d + 4 * n * vocab, n * vocab),
        compiler_params=params(), name="backward_h")(lg, emb, st, inv, hid, res)


def resid_body(dh_ref, hid_ref, res_ref, inv_ref, w_ref, out_ref):
    inv = inv_ref[...]
    nrm = (res_ref[...] + hid_ref[...].astype(jnp.float32)) * inv
    dn = dh_ref[...] * w_ref[...]
    out_ref[...] = inv * (dn - nrm * jnp.mean(dn * nrm, axis=-1, keepdims=True))


def resid_grad(dh, hid, res, inv, w):
    n, d = hid.shape
    blk = pl.BlockSpec((TB, d), lambda i: (i, 0))
    return pl.pallas_call(
        resid_body, grid=(n // TB,), out_shape=jax.ShapeDtypeStruct((n, d), jnp.float32),
        in_specs=[blk, blk, blk, pl.BlockSpec((TB, 1), lambda i: (i, 0)), whole((1, d))], out_specs=blk,
        cost_estimate=cost(8 * n * d, 14 * n * d), compiler_params=params(), name="resid_grad")(dh, hid, res, inv, w)


def dlogits(l, st, base, inv_n):
    row = lax.broadcasted_iota(jnp.int32, (l.shape[0], 1), 0).astype(jnp.float32)
    p = jnp.exp(l - st[0:1]) * st[1:2]
    return jnp.where(row == st[2:3] - base, p - inv_n, p).astype(jnp.bfloat16)


def nt(a, b):
    return lax.dot_general(a, b, NT, preferred_element_type=jnp.float32)


def nn(a, b):
    return lax.dot_general(a, b, NN, preferred_element_type=jnp.float32)


def plane_rows_body(np_, own, split, inv_n, off_ref, e_ref, st_ref, *refs):
    if own:
        lg_ref, hb_ref, refs = refs[0], refs[1], refs[2:]
    else:
        acc_ref, refs = refs[0], refs[2:]
    h_refs, refs = refs[:2 * np_], refs[2 * np_:]
    out_refs, refs = refs[:split], refs[split:]
    all_ref, buf, h_scr, sem = refs
    i = pl.program_id(0)
    half = buf.shape[1] // 2

    def load(k, slot):
        return [pltpu.make_async_copy(h_refs[2 * k + u], buf.at[slot, pl.ds(u * half, half)], sem.at[slot, u]) for u in range(2)]

    @pl.when(i == 0)
    def _():
        for c in load(0, 0):
            c.start()

    for k in range(1, np_):
        @pl.when(i + 1 == k)
        def _():
            for c in load(k, k % 2):
                c.start()

    base = off_ref[0].astype(jnp.float32)
    rh = R // 2

    @pl.when(i == 0)
    def _():
        for u in range(2):
            o, at = out_refs[u % split], 0 if split == 2 else u * rh
            if own:
                o[pl.ds(at, rh), :] = nn(dlogits(lg_ref[pl.ds(u * rh, rh), :], st_ref[0], base + u * rh, inv_n), hb_ref[...])
            else:
                o[pl.ds(at, rh), :] = acc_ref[pl.ds(u * rh, rh), :]

    slot = lax.rem(i, 2)
    for u in range(2):
        pltpu.make_async_copy(h_refs[u], buf.at[slot, pl.ds(u * half, half)], sem.at[slot, u]).wait()
    h_scr[...] = buf[slot].astype(jnp.bfloat16)
    all_ref[...] = h_scr[...]

    st = st_ref[i + own]
    ls = [nt(e_ref[pl.ds(u * rh, rh), :], h_scr[...]) for u in range(2)]
    for u in range(2):
        o, at = out_refs[u % split], 0 if split == 2 else u * rh
        o[pl.ds(at, rh), :] += nn(dlogits(ls[u], st, base + u * rh, inv_n), h_scr[...])


def plane_rows(off, emb, st, parts, inv_n, split, slots, own=None, acc=None, so_far=None):
    np_, (half, d) = len(parts) // 2, parts[0].shape
    n = 2 * half
    one = pl.Buffered(1)
    at = lambda i, off: (pl.multiple_of(off[0], 16), 0)
    whole_r = lambda r: pl.BlockSpec((r, d), lambda i, off: (0, 0), pipeline_mode=one)
    any_space = pl.BlockSpec(memory_space=pl.ANY)
    if own is not None:
        lead, specs = list(own), [pl.BlockSpec((pl.Element(R), pl.Element(n)), at, pipeline_mode=one), whole((n, d))]
    else:
        lead, specs = [acc, so_far], [whole_r(R), any_space]
    return pl.pallas_call(
        functools.partial(plane_rows_body, np_, int(own is not None), split, inv_n),
        out_shape=tuple([jax.ShapeDtypeStruct((R // split, d), jnp.float32)] * split + [jax.ShapeDtypeStruct((7, n, d), jnp.bfloat16)]),
        grid_spec=pltpu.PrefetchScalarGridSpec(
            num_scalar_prefetch=1, grid=(np_,),
            in_specs=[pl.BlockSpec((pl.Element(R, (0, R)), pl.Element(d)), at, pipeline_mode=one), whole(st.shape)] + specs
            + [any_space] * (2 * np_),
            out_specs=tuple([whole_r(R // split)] * split + [pl.BlockSpec((None, n, d), lambda i, off: (slots(i), 0, 0))]),
            scratch_shapes=[pltpu.VMEM((2, n, d), jnp.float32), pltpu.VMEM((n, d), jnp.bfloat16), pltpu.SemaphoreType.DMA((2, 2))]),
        input_output_aliases={} if own is not None else {4: split},
        cost_estimate=cost(4 * np_ * n * d * R, 6 * np_ * n * d, np_ * n * R),
        compiler_params=params(), name="plane_rows")(off, emb, st, *lead, *parts)


def chip_rows(off, lg, emb, st, hb, hs, slot, nb, inv_n):
    n, d = hb.shape

    def body(off_ref, lg_ref, e_ref, st_ref, h_ref, s_ref, out_ref):
        base = off_ref[1 + pl.program_id(0)].astype(jnp.float32)
        l = nt(e_ref[...], s_ref[...])
        out_ref[...] = nn(dlogits(lg_ref[...], st_ref[0], base, inv_n), h_ref[...])
        out_ref[...] += nn(dlogits(l, st_ref[1], base, inv_n), s_ref[...])

    at = lambda i, off: (pl.multiple_of(off[1 + i], 16), 0)
    return pl.pallas_call(
        body, out_shape=jax.ShapeDtypeStruct((nb * R, d), jnp.float32),
        grid_spec=pltpu.PrefetchScalarGridSpec(
            num_scalar_prefetch=1, grid=(nb,),
            in_specs=[pl.BlockSpec((pl.Element(R), pl.Element(n)), at), pl.BlockSpec((pl.Element(R, (0, R)), pl.Element(d)), at),
                      whole((8, 8, n)), whole((n, d)), pl.BlockSpec((None, n, d), lambda i, off: (slot, 0, 0), pipeline_mode=pl.Buffered(1))],
            out_specs=pl.BlockSpec((R, d), lambda i, off: (i, 0))),
        cost_estimate=cost(6 * n * d * nb * R, 8 * d * nb * R, 2 * n * nb * R),
        compiler_params=params(), name="chip_rows")(off, lg, emb, st, hb, hs)


def rest_rows(off, b0, nb, ng, emb, st, acc, hs, inv_n):
    n, d = hs.shape[1], hs.shape[2]

    def body(off_ref, e_ref, st_ref, h_ref, acc_ref, out_ref):
        i, j = pl.program_id(0), pl.program_id(1)
        base = off_ref[1 + b0 + i].astype(jnp.float32)
        l = nt(e_ref[...], h_ref[0])
        for q in range(2):
            after = nt(e_ref[...], h_ref[1]) if q == 0 else None
            x = nn(dlogits(l, st_ref[q], base, inv_n), h_ref[q])
            if q == 0:
                out_ref[...] = jnp.where(j == 0, acc_ref[...], out_ref[...]) + x
            else:
                out_ref[...] += x
            l = after

    return pl.pallas_call(
        body, out_shape=jax.ShapeDtypeStruct((nb * R, d), jnp.float32),
        grid_spec=pltpu.PrefetchScalarGridSpec(
            num_scalar_prefetch=1, grid=(nb, ng),
            in_specs=[pl.BlockSpec((pl.Element(R, (0, R)), pl.Element(d)), lambda i, j, off: (pl.multiple_of(off[1 + b0 + i], 16), 0)),
                      pl.BlockSpec((2, 8, n), lambda i, j, off: (j + 1, 0, 0)), pl.BlockSpec((2, n, d), lambda i, j, off: (j, 0, 0)),
                      pl.BlockSpec((R, d), lambda i, j, off: (b0 + i, 0))],
            out_specs=pl.BlockSpec((R, d), lambda i, j, off: (i, 0))),
        cost_estimate=cost(4 * 2 * ng * n * d * nb * R, 10 * d * nb * R, 2 * ng * n * nb * R),
        compiler_params=params(), name="rest_rows")(off, emb, st, hs, acc)


NBUF = 8
CH = 200


def place_body(jobs, pos_ref, *refs):
    srcs, out_ref, buf, isem, osem = refs[:-4], refs[-4], refs[-3], refs[-2], refs[-1]
    n = len(jobs)

    def fetch(j):
        s, r0, rows, _, _, _ = jobs[j]
        return pltpu.make_async_copy(srcs[s].at[pl.ds(r0, rows)], buf.at[j % NBUF, pl.ds(0, rows)], isem.at[j % NBUF])

    def put(j, rows):
        _, _, _, k, add, _ = jobs[j]
        at = pl.multiple_of(pos_ref[k] + add, 8)
        return pltpu.make_async_copy(buf.at[j % NBUF, pl.ds(0, rows)], out_ref.at[pl.ds(at, rows)], osem.at[j % NBUF])

    def each(j, f):
        _, _, rows, k, _, short = jobs[j]
        if short == rows:
            f(put(j, rows))
        else:
            last = pos_ref[k] == pos_ref[0]

            @pl.when(last)
            def _():
                if short > 0:
                    f(put(j, short))

            @pl.when(jnp.logical_not(last))
            def _():
                f(put(j, rows))

    lead = NBUF // 2
    for j in range(min(lead, n)):
        fetch(j).start()
    for j in range(n):
        fetch(j).wait()
        each(j, lambda c: c.start())
        nxt = j + lead
        if nxt < n:
            if nxt >= NBUF:
                each(nxt - NBUF, lambda c: c.wait())
            fetch(nxt).start()
    for j in range(max(0, n - NBUF), n):
        each(j, lambda c: c.wait())


def place(pos, pieces, vocab, d, tail, so_far=None):
    jobs, ops = [], []
    for arr, k, add, ends in pieces:
        ops.append(arr)
        for r0 in range(0, arr.shape[0], CH):
            rows = min(CH, arr.shape[0] - r0)
            short = max(0, min(rows, (tail - add - r0) // 8 * 8)) if ends else rows
            jobs.append((len(ops) - 1, r0, rows, k, add + r0, short))
    if so_far is not None:
        ops.append(so_far)
    return pl.pallas_call(
        functools.partial(place_body, jobs), out_shape=jax.ShapeDtypeStruct((vocab, d), jnp.float32),
        input_output_aliases={} if so_far is None else {len(ops): 0},
        grid_spec=pltpu.PrefetchScalarGridSpec(
            num_scalar_prefetch=1, grid=(), in_specs=[pl.BlockSpec(memory_space=pl.ANY)] * len(ops),
            out_specs=pl.BlockSpec(memory_space=pl.ANY),
            scratch_shapes=[pltpu.VMEM((NBUF, CH, d), jnp.float32), pltpu.SemaphoreType.DMA((NBUF,)), pltpu.SemaphoreType.DMA((NBUF,))]),
        cost_estimate=cost(1000, 8 * vocab * d), compiler_params=params(), name="place")(pos, *ops)


def place_tail(pos, own, other, row, out):
    vocab, d = out.shape

    def body(pos_ref, own_ref, other_ref, _, out_ref):
        out_ref[...] = jnp.where(pos_ref[9] == pos_ref[0], own_ref[...], other_ref[...])

    src = pl.BlockSpec((8, d), lambda i, pos: (row // 8, 0))
    return pl.pallas_call(
        body, out_shape=jax.ShapeDtypeStruct((vocab, d), jnp.float32),
        grid_spec=pltpu.PrefetchScalarGridSpec(
            num_scalar_prefetch=1, grid=(1,), in_specs=[src, src, pl.BlockSpec(memory_space=pl.ANY)],
            out_specs=pl.BlockSpec((8, d), lambda i, pos: (vocab // 8, 0))),
        input_output_aliases={3: 0}, compiler_params=params(), name="place_tail")(pos, own, other, out)


def solution(mesh):
    n_dp = mesh.shape['dp']

    def hop(dx, dy, dc):
        perm = []
        for i in range(n_dp):
            c, x, y = i % 2, (i // 2) % 2, i // 4
            perm.append((i, ((y ^ dy) * 2 + (x ^ dx)) * 2 + (c ^ dc)))
        return lambda a: lax.ppermute(a, 'dp', perm)

    over_x, over_y, over_c = hop(1, 0, 0), hop(0, 1, 0), hop(0, 0, 1)

    def program(hidden, residual, targets, embedding, norm_w):
        n_tok = hidden.shape[0] * hidden.shape[1]
        inv_n = 1.0 / n_tok

        def body(hid_loc, res_loc, tgt_loc, emb, norm_vec):
            _, n, d = hid_loc.shape
            hid, res = hid_loc.reshape(n, d), res_loc.reshape(n, d)
            vocab = emb.shape[0]
            w = norm_vec.reshape(1, d)
            tp, dp = lax.axis_index('tp'), lax.axis_index('dp')
            hb, inv, hf1 = norm_fwd(hid, res, w, 0)
            x1 = over_x(hf1)
            hb, inv, hf2 = norm_fwd(hid, res, w, 1, (hb, inv))
            y2 = over_y(hf2)
            x2, y1, s1, s2 = over_x(hf2), over_y(hf1), over_c(hf1), over_c(hf2)
            d1, d2 = over_y(x1), over_x(y2)
            xs1, ys2 = over_c(x1), over_c(y2)
            xs2, ys1 = over_c(x2), over_c(y1)
            ds1, ds2 = over_c(d1), over_c(d2)
            lg, st = forward(hb, emb)
            st = lax.all_gather(st[0:2], 'tp', axis=0)
            mx = jnp.max(st[:, 0], axis=0)
            sm = jnp.sum(st[:, 1] * jnp.exp(st[:, 0] - mx), axis=0)
            tgt = tgt_loc.reshape(n) - tp * vocab
            tgt = jnp.where((tgt >= 0) & (tgt < vocab), tgt, -1).astype(jnp.float32)
            mine = jnp.concatenate([jnp.stack([mx, inv_n / sm, tgt]), jnp.zeros((5, n), jnp.float32)], axis=0)
            dhg, hit = backward_h(lg, emb, mine, inv, hid, res, inv_n)
            own_loss = jnp.where(tp == 0, jnp.sum(mx + jnp.log(sm)), 0.0) - jnp.sum(hit)
            extra = jnp.concatenate([jnp.sum(dhg[n:], axis=0), jnp.full((n,), own_loss * inv_n)]).reshape(3, n)
            plane = lax.all_gather(jnp.concatenate([mine[0:3], extra, mine[6:8]], axis=0), 'dp', axis=0)
            sums = jnp.sum(plane[:, 3:6], axis=0).reshape(3 * n)
            top = jnp.concatenate([jnp.stack([sums[:d], jnp.broadcast_to(sums[2 * n], (d,))]), jnp.zeros((6, d), jnp.float32)], axis=0)
            dhg = lax.psum(lax.dynamic_update_slice(dhg, top, (n, 0)), 'tp')
            grad_w, loss = dhg[n], dhg[n + 1, 0]
            order = jnp.stack([dp ^ k for k in range(n_dp)])
            plane = plane[order]

            f0 = n_dp * R
            fh = NF * R
            core = dp % 2
            off = jnp.concatenate([jnp.stack([dp * R]), f0 + core * fh + R * jnp.arange(NF)]).astype(jnp.int32)
            gate = lax.optimization_barrier
            a, hs = plane_rows(off, emb, plane, [s1, s2, x1, x2, xs1, xs2, y1, y2, ys1, ys2], inv_n, 1, lambda i: lax.rem(i + 6, 7), own=(lg, hb))
            acc = chip_rows(off, lg, emb, plane, hb, hs, 6, NF, inv_n)
            a, _ = gate((a, acc))
            a1, a2, hs = plane_rows(off, emb, plane[6:8], [d1, d2, ds1, ds2], inv_n, 2, lambda i: i + 4, acc=a, so_far=hs)
            ax1, ay2 = over_x(a1), over_y(a2)
            ax2, ay1 = over_x(a2), over_y(a1)
            as1, as2 = over_c(a1), over_c(a2)
            ad1, ad2 = over_y(ax1), over_x(ay2)
            axs1, ays2 = over_c(ax1), over_c(ay2)
            axs2, ays1 = over_c(ax2), over_c(ay1)
            ads1, ads2 = over_c(ad1), over_c(ad2)
            pieces, last, j = [], a1, 0
            for k, (p1, p2) in enumerate([(a1, a2), (as1, as2), (ax1, ax2), (axs1, axs2), (ay1, ay2), (ays1, ays2), (ad1, ad2), (ads1, ads2)]):
                pieces += [(p1, 1 + k, 0, False), (p2, 1 + k, R // 2, False)]
            tail = vocab - f0 - fh
            for cnt in GROUPS:
                acc, last = gate((acc, last))
                last = rest_rows(off, j, cnt, 3, emb, plane, acc, hs, inv_n)
                other = over_c(last)
                pieces = [(last, 9, j * R, True), (other, 10, j * R, True)] + pieces
                if j * R <= tail < (j + cnt) * R:
                    ending = (last, other, tail // 8 * 8 - j * R)
                j += cnt
            pos = jnp.concatenate([jnp.stack([f0 + fh]), order * R, jnp.stack([f0 + core * fh, f0 + (1 - core) * fh])]).astype(jnp.int32)
            late = [p for p in pieces if p[0] is ads1 or p[0] is ads2 or p[0] is other]
            grad_emb = place(pos, [p for p in pieces if all(p[0] is not q[0] for q in late)], vocab, d, tail)
            grad_emb = place(pos, late, vocab, d, tail, grad_emb)
            if vocab % 8:
                grad_emb = place_tail(pos, *ending, grad_emb)
            grad_r = resid_grad(dhg, hid, res, inv, w)
            return loss, grad_r.reshape(hid_loc.shape), grad_emb, grad_w

        sharded = jax.shard_map(
            body, mesh=mesh,
            in_specs=(P('dp', None, None), P('dp', None, None), P('dp', None), P('tp', None), P(None)),
            out_specs=(P(), P('dp', None, None), P('tp', None), P(None)),
            check_vma=False)
        return sharded(hidden, residual, targets, embedding, norm_w)

    return program
```

```python
import functools

import jax
import jax.numpy as jnp
from jax import lax
from jax.experimental import pallas as pl
from jax.experimental.pallas import tpu as pltpu
from jax.sharding import PartitionSpec as P


EPS = 1e-5
NEG = -3.0e38
VMEM_CAP = 66 * 1024 * 1024
NT = (((1,), (1,)), ((), ()))
NN = (((1,), (0,)), ((), ()))
TN = (((0,), (0,)), ((), ()))
VB = 1280
SUB = 256
TB = 128
RA = 864
R = 576
NF = 5
GROUPS = (3, 2)


def params(**kw):
    return pltpu.CompilerParams(vmem_limit_bytes=VMEM_CAP, **kw)


def cost(flops, nbytes, exps=0):
    return pl.CostEstimate(flops=int(flops), bytes_accessed=int(nbytes), transcendentals=int(exps))


def whole(shape):
    return pl.BlockSpec(shape, lambda *a: (0,) * len(shape), pipeline_mode=pl.Buffered(1))


def norm_body(hid_ref, res_ref, w_ref, *refs):
    hb_ref, inv_ref, hf_ref = refs[-3:]
    r = res_ref[...] + hid_ref[...].astype(jnp.float32)
    inv = lax.rsqrt(jnp.mean(r * r, axis=-1, keepdims=True) + EPS)
    h = (r * inv * w_ref[...]).astype(jnp.bfloat16)
    hb_ref[...] = h
    hf_ref[...] = h.astype(jnp.float32)
    inv_ref[...] = inv


def norm_fwd(hid, res, w, half, so_far=()):
    n, d = hid.shape
    steps = n // (2 * TB)
    src = pl.BlockSpec((TB, d), lambda i: (i + half * steps, 0))
    return pl.pallas_call(
        norm_body, grid=(steps,),
        out_shape=(jax.ShapeDtypeStruct((n, d), jnp.bfloat16), jax.ShapeDtypeStruct((n, 1), jnp.float32),
                   jax.ShapeDtypeStruct((n // 2, d), jnp.float32)),
        in_specs=[src, src, whole((1, d))] + [pl.BlockSpec(memory_space=pl.ANY)] * len(so_far),
        out_specs=[src, pl.BlockSpec((TB, 1), lambda i: (i + half * steps, 0)), pl.BlockSpec((TB, d), lambda i: (i, 0))],
        input_output_aliases={3: 0, 4: 1} if so_far else {},
        cost_estimate=cost(8 * n * d, 6 * n * d), compiler_params=params(), name="norm_fwd")(hid, res, w, *so_far)


def fwd_body(vocab, h_ref, e_ref, lg_ref, st_ref, m_scr, s_scr):
    i = pl.program_id(0)
    n = h_ref.shape[0]

    @pl.when(i == 0)
    def _():
        m_scr[...] = jnp.full_like(m_scr, NEG)
        s_scr[...] = jnp.zeros_like(s_scr)

    def dot(k):
        return lax.dot_general(e_ref[pl.ds(k * SUB, SUB), :], h_ref[...], NT, preferred_element_type=jnp.float32)

    def stats(l, k):
        if (k + 1) * SUB > vocab % VB:
            row = lax.broadcasted_iota(jnp.int32, (SUB, 1), 0)
            l = jnp.where(row < vocab - i * VB - k * SUB, l, NEG)
        lg_ref[pl.ds(k * SUB, SUB), :] = l
        m_old = m_scr[...]
        l = l.reshape(SUB // 8, 8, n)
        m_new = jnp.maximum(m_old, jnp.max(l, axis=0))
        m_scr[...] = m_new
        s_scr[...] = s_scr[...] * jnp.exp(m_old - m_new) + jnp.sum(jnp.exp(l - m_new[None]), axis=0)

    l = dot(0)
    for k in range(VB // SUB):
        after = dot(k + 1) if (k + 1) * SUB < VB else None
        stats(l, k)
        l = after

    @pl.when(i == pl.num_programs(0) - 1)
    def _():
        m = m_scr[...]
        mx = jnp.max(m, axis=0, keepdims=True)
        sm = jnp.sum(s_scr[...] * jnp.exp(m - mx), axis=0, keepdims=True)
        row = lax.broadcasted_iota(jnp.int32, (8, 1), 0)
        st_ref[...] = jnp.where(row == 0, mx, sm)


def forward(h, emb):
    n, d = h.shape
    vocab = emb.shape[0]
    nb = pl.cdiv(vocab, VB)
    return pl.pallas_call(
        functools.partial(fwd_body, vocab), grid=(nb,),
        out_shape=(jax.ShapeDtypeStruct((nb * VB, n), jnp.float32), jax.ShapeDtypeStruct((8, n), jnp.float32)),
        in_specs=[whole((n, d)), pl.BlockSpec((VB, d), lambda i: (i, 0))],
        out_specs=[pl.BlockSpec((VB, n), lambda i: (i, 0)), pl.BlockSpec((8, n), lambda i: (0, 0))],
        scratch_shapes=[pltpu.VMEM((8, n), jnp.float32)] * 2,
        cost_estimate=cost(2 * n * d * vocab, 2 * vocab * d + 4 * n * vocab, n * vocab),
        compiler_params=params(), name="forward")(h, emb)


def dh_body(vocab, inv_n, lg_ref, e_ref, st_ref, inv_ref, hid_ref, res_ref, dh_ref, hid_scr, res_scr, t_scr, sem):
    i = pl.program_id(0)
    n = st_ref.shape[1]
    loads = [pltpu.make_async_copy(hid_ref, hid_scr, sem.at[0]), pltpu.make_async_copy(res_ref, res_scr, sem.at[1])]

    @pl.when(i == 0)
    def _():
        for c in loads:
            c.start()
        dh_ref[...] = jnp.zeros_like(dh_ref)
        t_scr[...] = jnp.zeros_like(t_scr)

    m, si = st_ref[0:1], st_ref[1:2]
    row = lax.broadcasted_iota(jnp.int32, (SUB, 1), 0)
    rowf = row.astype(jnp.float32)

    def dlogits(k):
        l = lg_ref[pl.ds(k * SUB, SUB), :]
        p = jnp.exp(l - m) * si
        hit = rowf == st_ref[2:3] - (i * VB + k * SUB).astype(jnp.float32)
        t = t_scr[...]
        for u in range(SUB // 8):
            t = jnp.where(hit[u * 8:(u + 1) * 8], l[u * 8:(u + 1) * 8], t)
        t_scr[...] = t
        return jnp.where(hit, p - inv_n, p).astype(jnp.bfloat16)

    g = dlogits(0)
    for k in range(VB // SUB):
        after = dlogits(k + 1) if (k + 1) * SUB < VB else None
        e = e_ref[pl.ds(k * SUB, SUB), :]
        if (k + 1) * SUB > vocab % VB:
            e = jnp.where(row < vocab - i * VB - k * SUB, e, 0)
        dh_ref[pl.ds(0, n), :] += lax.dot_general(g, e, TN, preferred_element_type=jnp.float32)
        g = after

    @pl.when(i == pl.num_programs(0) - 1)
    def _():
        for c in loads:
            c.wait()
        d = dh_ref.shape[1]
        once = (lax.broadcasted_iota(jnp.int32, (8, 1), 0) == 0) & (lax.axis_index('tp') == 0)
        lse = st_ref[0:1] + jnp.log(st_ref[3:4])
        dh_ref[pl.ds(n + 8, 8), pl.ds(0, n)] = jnp.where(once, lse, 0.0) - t_scr[...]
        dh_ref[pl.ds(n + 8, 8), pl.ds(n, d - n)] = jnp.zeros((8, d - n), jnp.float32)
        acc = jnp.zeros((8, d), jnp.float32)
        for q in range(n // TB):
            rows = pl.ds(q * TB, TB)
            v = dh_ref[rows, :] * ((res_scr[rows, :] + hid_scr[rows, :].astype(jnp.float32)) * inv_ref[rows, :])
            for u in range(TB // 8):
                acc = acc + v[u * 8:(u + 1) * 8]
        dh_ref[pl.ds(n, 8), :] = acc


def backward_h(lg, emb, st, inv, hid, res, inv_n):
    n, d = hid.shape
    vocab = emb.shape[0]
    any_space = pl.BlockSpec(memory_space=pl.ANY)
    return pl.pallas_call(
        functools.partial(dh_body, vocab, inv_n), grid=(lg.shape[0] // VB,),
        out_shape=jax.ShapeDtypeStruct((n + 16, d), jnp.float32),
        in_specs=[pl.BlockSpec((VB, n), lambda i: (i, 0)), pl.BlockSpec((VB, d), lambda i: (i, 0)), whole((8, n)), whole((n, 1)),
                  any_space, any_space],
        out_specs=whole((n + 16, d)),
        scratch_shapes=[pltpu.VMEM((n, d), jnp.bfloat16), pltpu.VMEM((n, d), jnp.float32), pltpu.VMEM((8, n), jnp.float32),
                        pltpu.SemaphoreType.DMA((2,))],
        cost_estimate=cost(2 * n * d * vocab, 2 * vocab * d + 4 * n * vocab, n * vocab),
        compiler_params=params(), name="backward_h")(lg, emb, st, inv, hid, res)


def resid_body(dh_ref, hid_ref, res_ref, inv_ref, w_ref, out_ref):
    inv = inv_ref[...]
    nrm = (res_ref[...] + hid_ref[...].astype(jnp.float32)) * inv
    dn = dh_ref[...] * w_ref[...]
    out_ref[...] = inv * (dn - nrm * jnp.mean(dn * nrm, axis=-1, keepdims=True))


def resid_grad(dh, hid, res, inv, w):
    n, d = hid.shape
    blk = pl.BlockSpec((TB, d), lambda i: (i, 0))
    return pl.pallas_call(
        resid_body, grid=(n // TB,), out_shape=jax.ShapeDtypeStruct((n, d), jnp.float32),
        in_specs=[blk, blk, blk, pl.BlockSpec((TB, 1), lambda i: (i, 0)), whole((1, d))], out_specs=blk,
        cost_estimate=cost(8 * n * d, 14 * n * d), compiler_params=params(), name="resid_grad")(dh, hid, res, inv, w)


MESH = pl.DeviceIdType.MESH


HOPS = ("", "c", "x", "y", "xc", "yc", "xy", "xyc")


def flipped(dp, hop):
    c, x, y = dp % 2, dp // 2 % 2, dp // 4
    x, y, c = [1 - v if name in hop else v for name, v in zip("xyc", (x, y, c))]
    return y * 4 + x * 2 + c


def meet(peers):
    barrier = pltpu.get_barrier_semaphore()
    for p in peers:
        pl.semaphore_signal(barrier, inc=1, device_id=p, device_id_type=MESH)
    pl.semaphore_wait(barrier, len(peers))


def stats_body(n_tp, vocab, inv_n, st_ref, tgt_ref, out_ref, got, send, recv):
    tp = lax.axis_index('tp')
    peers = [{'tp': (tp + k) % n_tp} for k in range(1, n_tp)]
    meet(peers)
    copies = [pltpu.make_async_remote_copy(src_ref=st_ref, dst_ref=got.at[k], send_sem=send.at[k], recv_sem=recv.at[k],
                                           device_id=p, device_id_type=MESH) for k, p in enumerate(peers)]
    for c in copies:
        c.start()
    for c in copies:
        c.wait()
    st = [st_ref[...]] + [got[k] for k in range(len(peers))]
    mx = functools.reduce(jnp.maximum, [v[0:1] for v in st])
    sm = sum(v[1:2] * jnp.exp(v[0:1] - mx) for v in st)
    t = tgt_ref[...] - (tp * vocab).astype(jnp.float32)
    t = jnp.where((t >= 0) & (t < vocab), t, -1.0)
    row = lax.broadcasted_iota(jnp.int32, (8, 1), 0)
    out_ref[...] = jnp.where(row == 0, mx, jnp.where(row == 1, inv_n / sm, jnp.where(row == 2, t, sm)))


def exchange_stats(st, tgt, n_tp, vocab, inv_n):
    n = st.shape[1]
    vm = pl.BlockSpec(memory_space=pltpu.VMEM)
    return pl.pallas_call(
        functools.partial(stats_body, n_tp, vocab, inv_n), out_shape=jax.ShapeDtypeStruct((8, n), jnp.float32),
        in_specs=[vm, vm], out_specs=vm,
        scratch_shapes=[pltpu.VMEM((n_tp - 1, 8, n), jnp.float32)] + [pltpu.SemaphoreType.DMA((n_tp - 1,))] * 2,
        compiler_params=pltpu.CompilerParams(collective_id=0, has_side_effects=True), name="exchange_stats")(st, tgt)


def dlogits(l, st, base, inv_n):
    row = lax.broadcasted_iota(jnp.int32, (l.shape[0], 1), 0).astype(jnp.float32)
    p = jnp.exp(l - st[0:1]) * st[1:2]
    return jnp.where(row == st[2:3] - base, p - inv_n, p).astype(jnp.bfloat16)


def nt(a, b):
    return lax.dot_general(a, b, NT, preferred_element_type=jnp.float32)


def nn(a, b):
    return lax.dot_general(a, b, NN, preferred_element_type=jnp.float32)


def plane_rows_body(nl, ns, own, split, inv_n, e_ref, st_ref, *refs):
    if own:
        lg_ref, hb_ref, refs = refs[0], refs[1], refs[2:]
    else:
        acc_ref, refs = refs[0], refs[2:]
    h_refs, refs = refs[:2 * nl], refs[2 * nl:]
    out_refs, refs = refs[:split], refs[split:]
    all_ref, refs = refs[0], refs[1:]
    if own:
        land, refs = refs[0], refs[1:]
    buf, h_scr, sem, send, recv = refs
    i = pl.program_id(0)
    half = buf.shape[1] // 2
    dp = lax.axis_index('dp')
    other = {'dp': flipped(dp, "c")}

    def load(k, slot):
        cs = []
        for u in range(2):
            src = h_refs[2 * k + u] if k < nl else land.at[k - nl, pl.ds(u * half, half)]
            cs.append(pltpu.make_async_copy(src, buf.at[slot, pl.ds(u * half, half)], sem.at[slot, u]))
        return cs

    def over(k):
        cs = []
        for u in range(2):
            dst = land.at[k, pl.ds(u * half, half)] if own else buf.at[1, pl.ds(u * half, half)]
            cs.append(pltpu.make_async_remote_copy(src_ref=h_refs[2 * (nl - ns + k) + u], dst_ref=dst, send_sem=send.at[k, u],
                                                   recv_sem=recv.at[k, u], device_id=other, device_id_type=MESH))
        return cs

    @pl.when(i == 0)
    def _():
        for c in load(0, 0):
            c.start()
        meet([other])
        for k in range(ns):
            for c in over(k):
                c.start()

    for k in range(1, nl + ns if own else nl):
        @pl.when(i + 1 == k)
        def _():
            if k >= nl:
                for c in over(k - nl):
                    c.wait_recv()
            for c in load(k, k % 2):
                c.start()

    base = (dp * RA).astype(jnp.float32)
    rh = RA // 2

    @pl.when(i == 0)
    def _():
        for u in range(2):
            o, at = out_refs[u % split], 0 if split == 2 else u * rh
            if own:
                o[pl.ds(at, rh), :] = nn(dlogits(lg_ref[pl.ds(u * rh, rh), :], st_ref[0], base + u * rh, inv_n), hb_ref[...])
            else:
                o[pl.ds(at, rh), :] = acc_ref[pl.ds(u * rh, rh), :]

    slot = lax.rem(i, 2)
    if own:
        for u in range(2):
            pltpu.make_async_copy(h_refs[u], buf.at[slot, pl.ds(u * half, half)], sem.at[slot, u]).wait()
    else:
        @pl.when(i == 0)
        def _():
            for c in load(0, 0):
                c.wait()

        @pl.when(i == 1)
        def _():
            for c in over(0):
                c.wait_recv()
    h_scr[...] = buf[slot].astype(jnp.bfloat16)
    all_ref[...] = h_scr[...]

    st = st_ref[i + own]
    ls = [nt(e_ref[pl.ds(u * rh, rh), :], h_scr[...]) for u in range(2)]
    for u in range(2):
        o, at = out_refs[u % split], 0 if split == 2 else u * rh
        o[pl.ds(at, rh), :] += nn(dlogits(ls[u], st, base + u * rh, inv_n), h_scr[...])

    @pl.when(i == nl + ns - 1)
    def _():
        for k in range(ns):
            for c in over(k):
                c.wait_send()


def plane_rows(emb, st, parts, ns, inv_n, split, slots, own=None, acc=None, so_far=None):
    nl, (half, d) = len(parts) // 2, parts[0].shape
    n, np_ = 2 * half, nl + ns
    one = pl.Buffered(1)
    at = lambda i: (lax.axis_index('dp'), 0)
    whole_r = lambda r: pl.BlockSpec((r, d), lambda i: (0, 0), pipeline_mode=one)
    any_space = pl.BlockSpec(memory_space=pl.ANY)
    out_shape = [jax.ShapeDtypeStruct((RA // split, d), jnp.float32)] * split + [jax.ShapeDtypeStruct((7, n, d), jnp.bfloat16)]
    out_specs = [whole_r(RA // split)] * split + [pl.BlockSpec((None, n, d), lambda i: (slots(i), 0, 0))]
    if own is not None:
        lead, specs = list(own), [pl.BlockSpec((RA, n), at, pipeline_mode=one), whole((n, d))]
        out_shape.append(jax.ShapeDtypeStruct((ns, n, d), jnp.float32))
        out_specs.append(any_space)
    else:
        lead, specs = [acc, so_far], [whole_r(RA), any_space]
    out = pl.pallas_call(
        functools.partial(plane_rows_body, nl, ns, int(own is not None), split, inv_n), grid=(np_,), out_shape=tuple(out_shape),
        in_specs=[pl.BlockSpec((RA, d), at, pipeline_mode=one),
                  whole((8, 8, n)) if own is not None else pl.BlockSpec((2, 8, n), lambda i: (3, 0, 0), pipeline_mode=one)] + specs + [any_space] * (2 * nl),
        out_specs=tuple(out_specs),
        scratch_shapes=[pltpu.VMEM((2, n, d), jnp.float32), pltpu.VMEM((n, d), jnp.bfloat16), pltpu.SemaphoreType.DMA((2, 2)),
                        pltpu.SemaphoreType.DMA((ns, 2)), pltpu.SemaphoreType.DMA((ns, 2))],
        input_output_aliases={} if own is not None else {3: split},
        cost_estimate=cost(4 * np_ * n * d * RA, 6 * np_ * n * d, np_ * n * RA),
        compiler_params=params(collective_id=2 + (own is None), has_side_effects=True), name="plane_rows")(emb, st, *lead, *parts)
    return out[:split + 1]


def chip_rows(off, lg, emb, st, hb, hs, slot, nb, inv_n):
    n, d = hb.shape

    def body(off_ref, lg_ref, e_ref, st_ref, h_ref, s_ref, out_ref):
        base = off_ref[pl.program_id(0)].astype(jnp.float32)
        l = nt(e_ref[...], s_ref[...])
        out_ref[...] = nn(dlogits(lg_ref[...], st_ref[0], base, inv_n), h_ref[...])
        out_ref[...] += nn(dlogits(l, st_ref[1], base, inv_n), s_ref[...])

    at = lambda i, off: (pl.multiple_of(off[i], 16), 0)
    return pl.pallas_call(
        body, out_shape=jax.ShapeDtypeStruct((nb * R, d), jnp.float32),
        grid_spec=pltpu.PrefetchScalarGridSpec(
            num_scalar_prefetch=1, grid=(nb,),
            in_specs=[pl.BlockSpec((pl.Element(R), pl.Element(n)), at), pl.BlockSpec((pl.Element(R, (0, R)), pl.Element(d)), at),
                      whole((8, 8, n)), whole((n, d)), pl.BlockSpec((None, n, d), lambda i, off: (slot, 0, 0), pipeline_mode=pl.Buffered(1))],
            out_specs=pl.BlockSpec((R, d), lambda i, off: (i, 0))),
        cost_estimate=cost(6 * n * d * nb * R, 8 * d * nb * R, 2 * n * nb * R),
        compiler_params=params(), name="chip_rows")(off, lg, emb, st, hb, hs)


def rest_rows(off, b0, nb, ng, emb, st, acc, hs, inv_n, out):
    n, d = hs.shape[1], hs.shape[2]
    vocab = emb.shape[0]
    ends = b0 + nb == NF
    short = (vocab - 8 * RA - (2 * NF - 1) * R) // 8 * 8

    def body(off_ref, e_ref, st_ref, h_ref, acc_ref, *refs):
        f_ref, out_ref, sem = refs[-3:]
        i, j = pl.program_id(0), pl.program_id(1)
        row0 = off_ref[b0 + i]
        base = row0.astype(jnp.float32)
        l = nt(e_ref[...], h_ref[0])
        for q in range(2):
            after = nt(e_ref[...], h_ref[1]) if q == 0 else None
            x = nn(dlogits(l, st_ref[q], base, inv_n), h_ref[q])
            if q == 0:
                f_ref[...] = jnp.where(j == 0, acc_ref[...], f_ref[...]) + x
            else:
                f_ref[...] += x
            l = after

        def put(rows, at=row0):
            return pltpu.make_async_copy(f_ref.at[pl.ds(0, rows)], out_ref.at[pl.ds(pl.multiple_of(at, 8), rows)], sem)

        @pl.when(j == ng - 1)
        def _():
            @pl.when(i > 0)
            def _():
                put(R, off_ref[b0 + i - 1]).wait()

            @pl.when(i < nb - 1)
            def _():
                put(R).start()

            @pl.when(i == nb - 1)
            def _():
                if ends:
                    past = row0 + R > vocab

                    @pl.when(past)
                    def _():
                        put(short).start()
                        put(short).wait()

                    @pl.when(jnp.logical_not(past))
                    def _():
                        put(R).start()
                        put(R).wait()
                else:
                    put(R).start()
                    put(R).wait()

    any_space = pl.BlockSpec(memory_space=pl.ANY)
    ops = [emb, st, hs, acc] + ([] if out is None else [out])
    return pl.pallas_call(
        body, out_shape=(jax.ShapeDtypeStruct((nb * R, d), jnp.float32), jax.ShapeDtypeStruct((vocab, d), jnp.float32)),
        grid_spec=pltpu.PrefetchScalarGridSpec(
            num_scalar_prefetch=1, grid=(nb, ng),
            in_specs=[pl.BlockSpec((pl.Element(R, (0, R)), pl.Element(d)), lambda i, j, off: (pl.multiple_of(off[b0 + i], 16), 0)),
                      pl.BlockSpec((2, 8, n), lambda i, j, off: (j + 1, 0, 0)), pl.BlockSpec((2, n, d), lambda i, j, off: (j, 0, 0)),
                      pl.BlockSpec((R, d), lambda i, j, off: (b0 + i, 0))] + [any_space] * (out is not None),
            out_specs=(pl.BlockSpec((R, d), lambda i, j, off: (i, 0)), any_space),
            scratch_shapes=[pltpu.SemaphoreType.DMA]),
        input_output_aliases={} if out is None else {5: 1},
        cost_estimate=cost(4 * 2 * ng * n * d * nb * R, 10 * d * nb * R, 2 * ng * n * nb * R),
        compiler_params=params(), name="rest_rows")(off, *ops)


NBUF = 8
CH = 216
LAST = 10


def place_body(jobs, pos_ref, *refs):
    srcs, out_ref, buf, isem, osem = refs[:-4], refs[-4], refs[-3], refs[-2], refs[-1]
    n = len(jobs)

    def fetch(j):
        s, r0, rows, _, _, _ = jobs[j]
        return pltpu.make_async_copy(srcs[s].at[pl.ds(r0, rows)], buf.at[j % NBUF, pl.ds(0, rows)], isem.at[j % NBUF])

    def put(j, rows):
        _, _, _, k, add, _ = jobs[j]
        at = pl.multiple_of(pos_ref[k] + add, 8)
        return pltpu.make_async_copy(buf.at[j % NBUF, pl.ds(0, rows)], out_ref.at[pl.ds(at, rows)], osem.at[j % NBUF])

    def each(j, f):
        _, _, rows, k, _, short = jobs[j]
        if short == rows:
            f(put(j, rows))
        else:
            last = pos_ref[k] == pos_ref[0]

            @pl.when(last)
            def _():
                if short > 0:
                    f(put(j, short))

            @pl.when(jnp.logical_not(last))
            def _():
                f(put(j, rows))

    lead = NBUF // 2
    for j in range(min(lead, n)):
        fetch(j).start()
    for j in range(n):
        fetch(j).wait()
        each(j, lambda c: c.start())
        nxt = j + lead
        if nxt < n:
            if nxt >= NBUF:
                each(nxt - NBUF, lambda c: c.wait())
            fetch(nxt).start()
    for j in range(max(0, n - NBUF), n):
        each(j, lambda c: c.wait())


def place(pos, pieces, vocab, d, tail, so_far=None):
    jobs, ops = [], []
    for arr, k, add in pieces:
        ops.append(arr)
        for r0 in range(0, arr.shape[0], CH):
            rows = min(CH, arr.shape[0] - r0)
            short = max(0, min(rows, (tail - add - r0) // 8 * 8)) if k == LAST else rows
            jobs.append((len(ops) - 1, r0, rows, k, add + r0, short))
    if so_far is not None:
        ops.append(so_far)
    return pl.pallas_call(
        functools.partial(place_body, jobs), out_shape=jax.ShapeDtypeStruct((vocab, d), jnp.float32),
        input_output_aliases={} if so_far is None else {len(ops): 0},
        grid_spec=pltpu.PrefetchScalarGridSpec(
            num_scalar_prefetch=1, grid=(), in_specs=[pl.BlockSpec(memory_space=pl.ANY)] * len(ops),
            out_specs=pl.BlockSpec(memory_space=pl.ANY),
            scratch_shapes=[pltpu.VMEM((NBUF, CH, d), jnp.float32), pltpu.SemaphoreType.DMA((NBUF,)), pltpu.SemaphoreType.DMA((NBUF,))]),
        cost_estimate=cost(1000, 8 * vocab * d), compiler_params=params(), name="place")(pos, *ops)


def place_tail(pos, own, other, row, out):
    vocab, d = out.shape

    def body(pos_ref, own_ref, other_ref, _, out_ref):
        out_ref[...] = jnp.where(pos_ref[9] == pos_ref[0], own_ref[...], other_ref[...])

    src = pl.BlockSpec((8, d), lambda i, pos: (row // 8, 0))
    return pl.pallas_call(
        body, out_shape=jax.ShapeDtypeStruct((vocab, d), jnp.float32),
        grid_spec=pltpu.PrefetchScalarGridSpec(
            num_scalar_prefetch=1, grid=(1,), in_specs=[src, src, pl.BlockSpec(memory_space=pl.ANY)],
            out_specs=pl.BlockSpec((8, d), lambda i, pos: (vocab // 8, 0))),
        input_output_aliases={3: 0}, compiler_params=params(), name="place_tail")(pos, own, other, out)


def solution(mesh):
    n_dp, n_tp = mesh.shape['dp'], mesh.shape['tp']

    def over(hop, a):
        return lax.ppermute(a, 'dp', [(i, flipped(i, hop)) for i in range(n_dp)])

    over_x, over_y, over_c = [functools.partial(over, hop) for hop in "xyc"]

    def program(hidden, residual, targets, embedding, norm_w):
        n_tok = hidden.shape[0] * hidden.shape[1]
        inv_n = 1.0 / n_tok

        def body(hid_loc, res_loc, tgt_loc, emb, norm_vec):
            _, n, d = hid_loc.shape
            hid, res = hid_loc.reshape(n, d), res_loc.reshape(n, d)
            vocab = emb.shape[0]
            w = norm_vec.reshape(1, d)
            dp = lax.axis_index('dp')
            hb, inv, hf1 = norm_fwd(hid, res, w, 0)
            x1 = over_x(hf1)
            hb, inv, hf2 = norm_fwd(hid, res, w, 1, (hb, inv))
            y2 = over_y(hf2)
            x2, y1 = over_x(hf2), over_y(hf1)
            s1, s2 = over_c(hf1), over_c(hf2)
            d1, d2 = over_y(x1), over_x(y2)
            lg, st = forward(hb, emb)
            mine = exchange_stats(st, tgt_loc.reshape(1, n).astype(jnp.float32), n_tp, vocab, inv_n)
            plane = jnp.stack([mine] + [over(hop, mine) for hop in HOPS[1:]])
            dhg = backward_h(lg, emb, mine, inv, hid, res, inv_n)
            dhg = lax.psum(dhg, 'tp')
            sums = jnp.concatenate([jnp.sum(dhg[n:n + 8], axis=0), jnp.full((n,), jnp.sum(dhg[n + 8:]) * inv_n)]).reshape(3 * n // 128, 128)
            for hop in "cxy":
                back = over(hop, sums)
                sums = sums + back
            sums = sums.reshape(3 * n)
            grad_w, loss = sums[:d], sums[2 * n]
            order = jnp.stack([flipped(dp, hop) for hop in HOPS])

            f0 = n_dp * RA
            fh = NF * R
            core = dp % 2
            off = (f0 + core * fh + R * jnp.arange(NF)).astype(jnp.int32)
            gate = lax.optimization_barrier
            a, hs = plane_rows(emb, plane, [s1, s2, x1, x2, y1, y2], 2, inv_n, 1, lambda i: lax.rem(i + 6, 7), own=(lg, hb))
            acc = chip_rows(off, lg, emb, plane, hb, hs, 6, NF, inv_n)
            a, _ = gate((a, acc))
            a1, a2, hs = plane_rows(emb, plane, [d1, d2], 1, inv_n, 2, lambda i: i + 4, acc=a, so_far=hs)
            ax1, ay2 = over_x(a1), over_y(a2)
            ax2, ay1 = over_x(a2), over_y(a1)
            as1, as2 = over_c(a1), over_c(a2)
            ad1, ad2 = over_y(ax1), over_x(ay2)
            axs1, ays2 = over_c(ax1), over_c(ay2)
            axs2, ays1 = over_c(ax2), over_c(ay1)
            ads1, ads2 = over_c(ad1), over_c(ad2)
            pieces, last, j = [], a1, 0
            for k, (p1, p2) in enumerate([(a1, a2), (as1, as2), (ax1, ax2), (ay1, ay2), (axs1, axs2), (ays1, ays2), (ad1, ad2), (ads1, ads2)]):
                pieces += [(p1, 1 + k, 0), (p2, 1 + k, RA // 2)]
            tail = vocab - f0 - fh
            grad_emb = None
            for cnt in GROUPS:
                acc, last = gate((acc, last))
                last, grad_emb = rest_rows(off, j, cnt, 3, emb, plane, acc, hs, inv_n, grad_emb)
                other = over_c(last)
                pieces = [(other, LAST, j * R)] + pieces
                if j * R <= tail < (j + cnt) * R:
                    ending = (last, other, tail // 8 * 8 - j * R)
                j += cnt
            pos = jnp.concatenate([jnp.stack([f0 + fh]), order * RA, jnp.stack([f0 + core * fh, f0 + (1 - core) * fh])]).astype(jnp.int32)

            def of(*arrays):
                return [p for p in pieces if any(p[0] is q for q in arrays)]

            early = [p for p in pieces if all(p[0] is not q for q in (axs2, ays1, ad1, ad2, ads1, ads2, other))]
            grad_emb = place(pos, early, vocab, d, tail, grad_emb)
            grad_r = resid_grad(dhg, hid, res, inv, w)
            grad_emb, grad_r = gate((grad_emb, grad_r))
            grad_emb = place(pos, of(other, axs2, ays1, ad1, ad2), vocab, d, tail, grad_emb)
            grad_emb = place(pos, of(ads1, ads2), vocab, d, tail, grad_emb)
            if vocab % 8:
                grad_emb = place_tail(pos, *ending, grad_emb)
            return loss, grad_r.reshape(hid_loc.shape), grad_emb, grad_w

        sharded = jax.shard_map(
            body, mesh=mesh,
            in_specs=(P('dp', None, None), P('dp', None, None), P('dp', None), P('tp', None), P(None)),
            out_specs=(P(), P('dp', None, None), P('tp', None), P(None)),
            check_vma=False)
        return sharded(hidden, residual, targets, embedding, norm_w)

    return program
```

```python
import functools

import jax
import jax.numpy as jnp
from jax import lax
from jax.experimental import pallas as pl
from jax.experimental.pallas import tpu as pltpu
from jax.sharding import PartitionSpec as P


EPS = 1e-5
NEG = -3.0e38
VMEM_CAP = 66 * 1024 * 1024
NT = (((1,), (1,)), ((), ()))
NN = (((1,), (0,)), ((), ()))
TN = (((0,), (0,)), ((), ()))
VB = 1280
SUB = 256
TB = 128
RA = 896
R = 544
NF = 5
GROUPS = (3, 2)


def params(**kw):
    return pltpu.CompilerParams(vmem_limit_bytes=VMEM_CAP, **kw)


def cost(flops, nbytes, exps=0):
    return pl.CostEstimate(flops=int(flops), bytes_accessed=int(nbytes), transcendentals=int(exps))


def whole(shape):
    return pl.BlockSpec(shape, lambda *a: (0,) * len(shape), pipeline_mode=pl.Buffered(1))


def norm_body(hid_ref, res_ref, w_ref, *refs):
    hb_ref, inv_ref, hf_ref = refs[-3:]
    r = res_ref[...] + hid_ref[...].astype(jnp.float32)
    inv = lax.rsqrt(jnp.mean(r * r, axis=-1, keepdims=True) + EPS)
    h = (r * inv * w_ref[...]).astype(jnp.bfloat16)
    hb_ref[...] = h
    hf_ref[...] = h.astype(jnp.float32)
    inv_ref[...] = inv


def norm_fwd(hid, res, w, half, so_far=()):
    n, d = hid.shape
    steps = n // (2 * TB)
    src = pl.BlockSpec((TB, d), lambda i: (i + half * steps, 0))
    return pl.pallas_call(
        norm_body, grid=(steps,),
        out_shape=(jax.ShapeDtypeStruct((n, d), jnp.bfloat16), jax.ShapeDtypeStruct((n, 1), jnp.float32),
                   jax.ShapeDtypeStruct((n // 2, d), jnp.float32)),
        in_specs=[src, src, whole((1, d))] + [pl.BlockSpec(memory_space=pl.ANY)] * len(so_far),
        out_specs=[src, pl.BlockSpec((TB, 1), lambda i: (i + half * steps, 0)), pl.BlockSpec((TB, d), lambda i: (i, 0))],
        input_output_aliases={3: 0, 4: 1} if so_far else {},
        cost_estimate=cost(8 * n * d, 6 * n * d), compiler_params=params(), name="norm_fwd")(hid, res, w, *so_far)


def fwd_body(vocab, h_ref, e_ref, lg_ref, st_ref, m_scr, s_scr):
    i = pl.program_id(0)
    n = h_ref.shape[0]

    @pl.when(i == 0)
    def _():
        m_scr[...] = jnp.full_like(m_scr, NEG)
        s_scr[...] = jnp.zeros_like(s_scr)

    def dot(k):
        return lax.dot_general(e_ref[pl.ds(k * SUB, SUB), :], h_ref[...], NT, preferred_element_type=jnp.float32)

    def stats(l, k):
        if (k + 1) * SUB > vocab % VB:
            row = lax.broadcasted_iota(jnp.int32, (SUB, 1), 0)
            l = jnp.where(row < vocab - i * VB - k * SUB, l, NEG)
        lg_ref[pl.ds(k * SUB, SUB), :] = l
        m_old = m_scr[...]
        l = l.reshape(SUB // 8, 8, n)
        m_new = jnp.maximum(m_old, jnp.max(l, axis=0))
        m_scr[...] = m_new
        s_scr[...] = s_scr[...] * jnp.exp(m_old - m_new) + jnp.sum(jnp.exp(l - m_new[None]), axis=0)

    l = dot(0)
    for k in range(VB // SUB):
        after = dot(k + 1) if (k + 1) * SUB < VB else None
        stats(l, k)
        l = after

    @pl.when(i == pl.num_programs(0) - 1)
    def _():
        m = m_scr[...]
        mx = jnp.max(m, axis=0, keepdims=True)
        sm = jnp.sum(s_scr[...] * jnp.exp(m - mx), axis=0, keepdims=True)
        row = lax.broadcasted_iota(jnp.int32, (8, 1), 0)
        st_ref[...] = jnp.where(row == 0, mx, sm)


def forward(h, emb):
    n, d = h.shape
    vocab = emb.shape[0]
    nb = pl.cdiv(vocab, VB)
    return pl.pallas_call(
        functools.partial(fwd_body, vocab), grid=(nb,),
        out_shape=(jax.ShapeDtypeStruct((nb * VB, n), jnp.float32), jax.ShapeDtypeStruct((8, n), jnp.float32)),
        in_specs=[whole((n, d)), pl.BlockSpec((VB, d), lambda i: (i, 0))],
        out_specs=[pl.BlockSpec((VB, n), lambda i: (i, 0)), pl.BlockSpec((8, n), lambda i: (0, 0))],
        scratch_shapes=[pltpu.VMEM((8, n), jnp.float32)] * 2,
        cost_estimate=cost(2 * n * d * vocab, 2 * vocab * d + 4 * n * vocab, n * vocab),
        compiler_params=params(), name="forward")(h, emb)


def dh_body(vocab, inv_n, lg_ref, e_ref, st_ref, inv_ref, hid_ref, res_ref, dh_ref, hid_scr, res_scr, t_scr, sem):
    i = pl.program_id(0)
    n = st_ref.shape[1]
    loads = [pltpu.make_async_copy(hid_ref, hid_scr, sem.at[0]), pltpu.make_async_copy(res_ref, res_scr, sem.at[1])]

    @pl.when(i == 0)
    def _():
        for c in loads:
            c.start()
        dh_ref[...] = jnp.zeros_like(dh_ref)
        t_scr[...] = jnp.zeros_like(t_scr)

    m, si = st_ref[0:1], st_ref[1:2]
    row = lax.broadcasted_iota(jnp.int32, (SUB, 1), 0)
    rowf = row.astype(jnp.float32)

    def dlogits(k):
        l = lg_ref[pl.ds(k * SUB, SUB), :]
        p = jnp.exp(l - m) * si
        hit = rowf == st_ref[2:3] - (i * VB + k * SUB).astype(jnp.float32)
        t = t_scr[...]
        for u in range(SUB // 8):
            t = jnp.where(hit[u * 8:(u + 1) * 8], l[u * 8:(u + 1) * 8], t)
        t_scr[...] = t
        return jnp.where(hit, p - inv_n, p).astype(jnp.bfloat16)

    g = dlogits(0)
    for k in range(VB // SUB):
        after = dlogits(k + 1) if (k + 1) * SUB < VB else None
        e = e_ref[pl.ds(k * SUB, SUB), :]
        if (k + 1) * SUB > vocab % VB:
            e = jnp.where(row < vocab - i * VB - k * SUB, e, 0)
        dh_ref[pl.ds(0, n), :] += lax.dot_general(g, e, TN, preferred_element_type=jnp.float32)
        g = after

    @pl.when(i == pl.num_programs(0) - 1)
    def _():
        for c in loads:
            c.wait()
        d = dh_ref.shape[1]
        once = (lax.broadcasted_iota(jnp.int32, (8, 1), 0) == 0) & (lax.axis_index('tp') == 0)
        lse = st_ref[0:1] + jnp.log(st_ref[3:4])
        dh_ref[pl.ds(n + 8, 8), pl.ds(0, n)] = jnp.where(once, lse, 0.0) - t_scr[...]
        dh_ref[pl.ds(n + 8, 8), pl.ds(n, d - n)] = jnp.zeros((8, d - n), jnp.float32)
        acc = jnp.zeros((8, d), jnp.float32)
        for q in range(n // TB):
            rows = pl.ds(q * TB, TB)
            v = dh_ref[rows, :] * ((res_scr[rows, :] + hid_scr[rows, :].astype(jnp.float32)) * inv_ref[rows, :])
            for u in range(TB // 8):
                acc = acc + v[u * 8:(u + 1) * 8]
        dh_ref[pl.ds(n, 8), :] = acc


def backward_h(lg, emb, st, inv, hid, res, inv_n):
    n, d = hid.shape
    vocab = emb.shape[0]
    any_space = pl.BlockSpec(memory_space=pl.ANY)
    return pl.pallas_call(
        functools.partial(dh_body, vocab, inv_n), grid=(lg.shape[0] // VB,),
        out_shape=jax.ShapeDtypeStruct((n + 16, d), jnp.float32),
        in_specs=[pl.BlockSpec((VB, n), lambda i: (i, 0)), pl.BlockSpec((VB, d), lambda i: (i, 0)), whole((8, n)), whole((n, 1)),
                  any_space, any_space],
        out_specs=whole((n + 16, d)),
        scratch_shapes=[pltpu.VMEM((n, d), jnp.bfloat16), pltpu.VMEM((n, d), jnp.float32), pltpu.VMEM((8, n), jnp.float32),
                        pltpu.SemaphoreType.DMA((2,))],
        cost_estimate=cost(2 * n * d * vocab, 2 * vocab * d + 4 * n * vocab, n * vocab),
        compiler_params=params(), name="backward_h")(lg, emb, st, inv, hid, res)


def resid_body(dh_ref, hid_ref, res_ref, inv_ref, w_ref, out_ref):
    inv = inv_ref[...]
    nrm = (res_ref[...] + hid_ref[...].astype(jnp.float32)) * inv
    dn = dh_ref[...] * w_ref[...]
    out_ref[...] = inv * (dn - nrm * jnp.mean(dn * nrm, axis=-1, keepdims=True))


def resid_grad(dh, hid, res, inv, w):
    n, d = hid.shape
    blk = pl.BlockSpec((TB, d), lambda i: (i, 0))
    return pl.pallas_call(
        resid_body, grid=(n // TB,), out_shape=jax.ShapeDtypeStruct((n, d), jnp.float32),
        in_specs=[blk, blk, blk, pl.BlockSpec((TB, 1), lambda i: (i, 0)), whole((1, d))], out_specs=blk,
        cost_estimate=cost(8 * n * d, 14 * n * d), compiler_params=params(), name="resid_grad")(dh, hid, res, inv, w)


MESH = pl.DeviceIdType.MESH


HOPS = ("", "c", "x", "y", "xc", "yc", "xy", "xyc")


def flipped(dp, hop):
    c, x, y = dp % 2, dp // 2 % 2, dp // 4
    x, y, c = [1 - v if name in hop else v for name, v in zip("xyc", (x, y, c))]
    return y * 4 + x * 2 + c


def meet(peers):
    barrier = pltpu.get_barrier_semaphore()
    for p in peers:
        pl.semaphore_signal(barrier, inc=1, device_id=p, device_id_type=MESH)
    pl.semaphore_wait(barrier, len(peers))


def stats_body(n_tp, vocab, inv_n, st_ref, tgt_ref, out_ref, got, send, recv):
    tp = lax.axis_index('tp')
    peers = [{'tp': (tp + k) % n_tp} for k in range(1, n_tp)]
    meet(peers)
    copies = [pltpu.make_async_remote_copy(src_ref=st_ref, dst_ref=got.at[k], send_sem=send.at[k], recv_sem=recv.at[k],
                                           device_id=p, device_id_type=MESH) for k, p in enumerate(peers)]
    for c in copies:
        c.start()
    for c in copies:
        c.wait()
    st = [st_ref[...]] + [got[k] for k in range(len(peers))]
    mx = functools.reduce(jnp.maximum, [v[0:1] for v in st])
    sm = sum(v[1:2] * jnp.exp(v[0:1] - mx) for v in st)
    t = tgt_ref[...] - (tp * vocab).astype(jnp.float32)
    t = jnp.where((t >= 0) & (t < vocab), t, -1.0)
    row = lax.broadcasted_iota(jnp.int32, (8, 1), 0)
    out_ref[...] = jnp.where(row == 0, mx, jnp.where(row == 1, inv_n / sm, jnp.where(row == 2, t, sm)))


def exchange_stats(st, tgt, n_tp, vocab, inv_n):
    n = st.shape[1]
    vm = pl.BlockSpec(memory_space=pltpu.VMEM)
    return pl.pallas_call(
        functools.partial(stats_body, n_tp, vocab, inv_n), out_shape=jax.ShapeDtypeStruct((8, n), jnp.float32),
        in_specs=[vm, vm], out_specs=vm,
        scratch_shapes=[pltpu.VMEM((n_tp - 1, 8, n), jnp.float32)] + [pltpu.SemaphoreType.DMA((n_tp - 1,))] * 2,
        compiler_params=pltpu.CompilerParams(collective_id=0, has_side_effects=True), name="exchange_stats")(st, tgt)


def dlogits(l, st, base, inv_n):
    row = lax.broadcasted_iota(jnp.int32, (l.shape[0], 1), 0).astype(jnp.float32)
    p = jnp.exp(l - st[0:1]) * st[1:2]
    return jnp.where(row == st[2:3] - base, p - inv_n, p).astype(jnp.bfloat16)


def nt(a, b):
    return lax.dot_general(a, b, NT, preferred_element_type=jnp.float32)


def nn(a, b):
    return lax.dot_general(a, b, NN, preferred_element_type=jnp.float32)


def plane_rows_body(nl, ns, own, split, inv_n, e_ref, st_ref, *refs):
    if own:
        lg_ref, hb_ref, refs = refs[0], refs[1], refs[2:]
    else:
        acc_ref, refs = refs[0], refs[2:]
    h_refs, refs = refs[:2 * nl], refs[2 * nl:]
    out_refs, refs = refs[:split], refs[split:]
    all_ref, refs = refs[0], refs[1:]
    if own:
        land, refs = refs[0], refs[1:]
    buf, h_scr, sem, send, recv = refs
    i = pl.program_id(0)
    half = buf.shape[1] // 2
    dp = lax.axis_index('dp')
    other = {'dp': flipped(dp, "c")}

    def load(k, slot):
        cs = []
        for u in range(2):
            src = h_refs[2 * k + u] if k < nl else land.at[k - nl, pl.ds(u * half, half)]
            cs.append(pltpu.make_async_copy(src, buf.at[slot, pl.ds(u * half, half)], sem.at[slot, u]))
        return cs

    def over(k):
        cs = []
        for u in range(2):
            dst = land.at[k, pl.ds(u * half, half)] if own else buf.at[1, pl.ds(u * half, half)]
            cs.append(pltpu.make_async_remote_copy(src_ref=h_refs[2 * (nl - ns + k) + u], dst_ref=dst, send_sem=send.at[k, u],
                                                   recv_sem=recv.at[k, u], device_id=other, device_id_type=MESH))
        return cs

    @pl.when(i == 0)
    def _():
        for c in load(0, 0):
            c.start()
        meet([other])
        for k in range(ns):
            for c in over(k):
                c.start()

    for k in range(1, nl + ns if own else nl):
        @pl.when(i + 1 == k)
        def _():
            if k >= nl:
                for c in over(k - nl):
                    c.wait_recv()
            for c in load(k, k % 2):
                c.start()

    base = (dp * RA).astype(jnp.float32)
    rh = RA // 2

    @pl.when(i == 0)
    def _():
        for u in range(2):
            o, at = out_refs[u % split], 0 if split == 2 else u * rh
            if own:
                o[pl.ds(at, rh), :] = nn(dlogits(lg_ref[pl.ds(u * rh, rh), :], st_ref[0], base + u * rh, inv_n), hb_ref[...])
            else:
                o[pl.ds(at, rh), :] = acc_ref[pl.ds(u * rh, rh), :]

    slot = lax.rem(i, 2)
    if own:
        for u in range(2):
            pltpu.make_async_copy(h_refs[u], buf.at[slot, pl.ds(u * half, half)], sem.at[slot, u]).wait()
    else:
        @pl.when(i == 0)
        def _():
            for c in load(0, 0):
                c.wait()

        @pl.when(i == 1)
        def _():
            for c in over(0):
                c.wait_recv()
    h_scr[...] = buf[slot].astype(jnp.bfloat16)
    all_ref[...] = h_scr[...]

    st = st_ref[i + own]
    ls = [nt(e_ref[pl.ds(u * rh, rh), :], h_scr[...]) for u in range(2)]
    for u in range(2):
        o, at = out_refs[u % split], 0 if split == 2 else u * rh
        o[pl.ds(at, rh), :] += nn(dlogits(ls[u], st, base + u * rh, inv_n), h_scr[...])

    @pl.when(i == nl + ns - 1)
    def _():
        for k in range(ns):
            for c in over(k):
                c.wait_send()


def plane_rows(emb, st, parts, ns, inv_n, split, slots, own=None, acc=None, so_far=None):
    nl, (half, d) = len(parts) // 2, parts[0].shape
    n, np_ = 2 * half, nl + ns
    one = pl.Buffered(1)
    at = lambda i: (lax.axis_index('dp'), 0)
    whole_r = lambda r: pl.BlockSpec((r, d), lambda i: (0, 0), pipeline_mode=one)
    any_space = pl.BlockSpec(memory_space=pl.ANY)
    out_shape = [jax.ShapeDtypeStruct((RA // split, d), jnp.float32)] * split + [jax.ShapeDtypeStruct((7, n, d), jnp.bfloat16)]
    out_specs = [whole_r(RA // split)] * split + [pl.BlockSpec((None, n, d), lambda i: (slots(i), 0, 0))]
    if own is not None:
        lead, specs = list(own), [pl.BlockSpec((RA, n), at, pipeline_mode=one), whole((n, d))]
        out_shape.append(jax.ShapeDtypeStruct((ns, n, d), jnp.float32))
        out_specs.append(any_space)
    else:
        lead, specs = [acc, so_far], [whole_r(RA), any_space]
    out = pl.pallas_call(
        functools.partial(plane_rows_body, nl, ns, int(own is not None), split, inv_n), grid=(np_,), out_shape=tuple(out_shape),
        in_specs=[pl.BlockSpec((RA, d), at, pipeline_mode=one),
                  whole((8, 8, n)) if own is not None else pl.BlockSpec((2, 8, n), lambda i: (3, 0, 0), pipeline_mode=one)] + specs + [any_space] * (2 * nl),
        out_specs=tuple(out_specs),
        scratch_shapes=[pltpu.VMEM((2, n, d), jnp.float32), pltpu.VMEM((n, d), jnp.bfloat16), pltpu.SemaphoreType.DMA((2, 2)),
                        pltpu.SemaphoreType.DMA((ns, 2)), pltpu.SemaphoreType.DMA((ns, 2))],
        input_output_aliases={} if own is not None else {3: split},
        cost_estimate=cost(4 * np_ * n * d * RA, 6 * np_ * n * d, np_ * n * RA),
        compiler_params=params(collective_id=2 + (own is None), has_side_effects=True), name="plane_rows")(emb, st, *lead, *parts)
    return out[:split + 1]


def chip_rows(off, lg, emb, st, hb, hs, slot, nb, inv_n):
    n, d = hb.shape

    def body(off_ref, lg_ref, e_ref, st_ref, h_ref, s_ref, out_ref):
        base = off_ref[pl.program_id(0)].astype(jnp.float32)
        l = nt(e_ref[...], s_ref[...])
        out_ref[...] = nn(dlogits(lg_ref[...], st_ref[0], base, inv_n), h_ref[...])
        out_ref[...] += nn(dlogits(l, st_ref[1], base, inv_n), s_ref[...])

    at = lambda i, off: (pl.multiple_of(off[i], 16), 0)
    return pl.pallas_call(
        body, out_shape=jax.ShapeDtypeStruct((nb * R, d), jnp.float32),
        grid_spec=pltpu.PrefetchScalarGridSpec(
            num_scalar_prefetch=1, grid=(nb,),
            in_specs=[pl.BlockSpec((pl.Element(R), pl.Element(n)), at), pl.BlockSpec((pl.Element(R, (0, R)), pl.Element(d)), at),
                      whole((8, 8, n)), whole((n, d)), pl.BlockSpec((None, n, d), lambda i, off: (slot, 0, 0), pipeline_mode=pl.Buffered(1))],
            out_specs=pl.BlockSpec((R, d), lambda i, off: (i, 0))),
        cost_estimate=cost(6 * n * d * nb * R, 8 * d * nb * R, 2 * n * nb * R),
        compiler_params=params(), name="chip_rows")(off, lg, emb, st, hb, hs)


def rest_rows(off, b0, nb, ng, emb, st, acc, hs, inv_n, out):
    n, d = hs.shape[1], hs.shape[2]
    vocab = emb.shape[0]
    ends = b0 + nb == NF
    short = (vocab - 8 * RA - (2 * NF - 1) * R) // 8 * 8

    def body(off_ref, e_ref, st_ref, h_ref, acc_ref, *refs):
        f_ref, out_ref, sem = refs[-3:]
        i, j = pl.program_id(0), pl.program_id(1)
        row0 = off_ref[b0 + i]
        base = row0.astype(jnp.float32)
        l = nt(e_ref[...], h_ref[0])
        for q in range(2):
            after = nt(e_ref[...], h_ref[1]) if q == 0 else None
            x = nn(dlogits(l, st_ref[q], base, inv_n), h_ref[q])
            if q == 0:
                f_ref[...] = jnp.where(j == 0, acc_ref[...], f_ref[...]) + x
            else:
                f_ref[...] += x
            l = after

        def put(rows, at=row0):
            return pltpu.make_async_copy(f_ref.at[pl.ds(0, rows)], out_ref.at[pl.ds(pl.multiple_of(at, 8), rows)], sem)

        @pl.when(j == ng - 1)
        def _():
            @pl.when(i > 0)
            def _():
                put(R, off_ref[b0 + i - 1]).wait()

            @pl.when(i < nb - 1)
            def _():
                put(R).start()

            @pl.when(i == nb - 1)
            def _():
                if ends:
                    past = row0 + R > vocab

                    @pl.when(past)
                    def _():
                        put(short).start()
                        put(short).wait()

                    @pl.when(jnp.logical_not(past))
                    def _():
                        put(R).start()
                        put(R).wait()
                else:
                    put(R).start()
                    put(R).wait()

    any_space = pl.BlockSpec(memory_space=pl.ANY)
    ops = [emb, st, hs, acc] + ([] if out is None else [out])
    return pl.pallas_call(
        body, out_shape=(jax.ShapeDtypeStruct((nb * R, d), jnp.float32), jax.ShapeDtypeStruct((vocab, d), jnp.float32)),
        grid_spec=pltpu.PrefetchScalarGridSpec(
            num_scalar_prefetch=1, grid=(nb, ng),
            in_specs=[pl.BlockSpec((pl.Element(R, (0, R)), pl.Element(d)), lambda i, j, off: (pl.multiple_of(off[b0 + i], 16), 0)),
                      pl.BlockSpec((2, 8, n), lambda i, j, off: (j + 1, 0, 0)), pl.BlockSpec((2, n, d), lambda i, j, off: (j, 0, 0)),
                      pl.BlockSpec((R, d), lambda i, j, off: (b0 + i, 0))] + [any_space] * (out is not None),
            out_specs=(pl.BlockSpec((R, d), lambda i, j, off: (i, 0)), any_space),
            scratch_shapes=[pltpu.SemaphoreType.DMA]),
        input_output_aliases={} if out is None else {5: 1},
        cost_estimate=cost(4 * 2 * ng * n * d * nb * R, 10 * d * nb * R, 2 * ng * n * nb * R),
        compiler_params=params(), name="rest_rows")(off, *ops)


NBUF = 8
CH = 224
LAST = 10


def place_body(jobs, pos_ref, *refs):
    srcs, out_ref, buf, isem, osem = refs[:-4], refs[-4], refs[-3], refs[-2], refs[-1]
    n = len(jobs)

    def fetch(j):
        s, r0, rows, _, _, _ = jobs[j]
        return pltpu.make_async_copy(srcs[s].at[pl.ds(r0, rows)], buf.at[j % NBUF, pl.ds(0, rows)], isem.at[j % NBUF])

    def put(j, rows):
        _, _, _, k, add, _ = jobs[j]
        at = pl.multiple_of(pos_ref[k] + add, 8)
        return pltpu.make_async_copy(buf.at[j % NBUF, pl.ds(0, rows)], out_ref.at[pl.ds(at, rows)], osem.at[j % NBUF])

    def each(j, f):
        _, _, rows, k, _, short = jobs[j]
        if short == rows:
            f(put(j, rows))
        else:
            last = pos_ref[k] == pos_ref[0]

            @pl.when(last)
            def _():
                if short > 0:
                    f(put(j, short))

            @pl.when(jnp.logical_not(last))
            def _():
                f(put(j, rows))

    lead = NBUF // 2
    for j in range(min(lead, n)):
        fetch(j).start()
    for j in range(n):
        fetch(j).wait()
        each(j, lambda c: c.start())
        nxt = j + lead
        if nxt < n:
            if nxt >= NBUF:
                each(nxt - NBUF, lambda c: c.wait())
            fetch(nxt).start()
    for j in range(max(0, n - NBUF), n):
        each(j, lambda c: c.wait())


def place(pos, pieces, vocab, d, tail, so_far=None):
    jobs, ops = [], []
    for arr, k, add in pieces:
        ops.append(arr)
        for r0 in range(0, arr.shape[0], CH):
            rows = min(CH, arr.shape[0] - r0)
            short = max(0, min(rows, (tail - add - r0) // 8 * 8)) if k == LAST else rows
            jobs.append((len(ops) - 1, r0, rows, k, add + r0, short))
    if so_far is not None:
        ops.append(so_far)
    return pl.pallas_call(
        functools.partial(place_body, jobs), out_shape=jax.ShapeDtypeStruct((vocab, d), jnp.float32),
        input_output_aliases={} if so_far is None else {len(ops): 0},
        grid_spec=pltpu.PrefetchScalarGridSpec(
            num_scalar_prefetch=1, grid=(), in_specs=[pl.BlockSpec(memory_space=pl.ANY)] * len(ops),
            out_specs=pl.BlockSpec(memory_space=pl.ANY),
            scratch_shapes=[pltpu.VMEM((NBUF, CH, d), jnp.float32), pltpu.SemaphoreType.DMA((NBUF,)), pltpu.SemaphoreType.DMA((NBUF,))]),
        cost_estimate=cost(1000, 8 * vocab * d), compiler_params=params(), name="place")(pos, *ops)


def place_tail(pos, own, other, row, out):
    vocab, d = out.shape

    def body(pos_ref, own_ref, other_ref, _, out_ref):
        out_ref[...] = jnp.where(pos_ref[9] == pos_ref[0], own_ref[...], other_ref[...])

    src = pl.BlockSpec((8, d), lambda i, pos: (row // 8, 0))
    return pl.pallas_call(
        body, out_shape=jax.ShapeDtypeStruct((vocab, d), jnp.float32),
        grid_spec=pltpu.PrefetchScalarGridSpec(
            num_scalar_prefetch=1, grid=(1,), in_specs=[src, src, pl.BlockSpec(memory_space=pl.ANY)],
            out_specs=pl.BlockSpec((8, d), lambda i, pos: (vocab // 8, 0))),
        input_output_aliases={3: 0}, compiler_params=params(), name="place_tail")(pos, own, other, out)


def solution(mesh):
    n_dp, n_tp = mesh.shape['dp'], mesh.shape['tp']

    def over(hop, a):
        return lax.ppermute(a, 'dp', [(i, flipped(i, hop)) for i in range(n_dp)])

    over_x, over_y, over_c = [functools.partial(over, hop) for hop in "xyc"]

    def program(hidden, residual, targets, embedding, norm_w):
        n_tok = hidden.shape[0] * hidden.shape[1]
        inv_n = 1.0 / n_tok

        def body(hid_loc, res_loc, tgt_loc, emb, norm_vec):
            _, n, d = hid_loc.shape
            hid, res = hid_loc.reshape(n, d), res_loc.reshape(n, d)
            vocab = emb.shape[0]
            w = norm_vec.reshape(1, d)
            dp = lax.axis_index('dp')
            hb, inv, hf1 = norm_fwd(hid, res, w, 0)
            x1 = over_x(hf1)
            hb, inv, hf2 = norm_fwd(hid, res, w, 1, (hb, inv))
            y2 = over_y(hf2)
            x2, y1 = over_x(hf2), over_y(hf1)
            s1, s2 = over_c(hf1), over_c(hf2)
            d1, d2 = over_y(x1), over_x(y2)
            lg, st = forward(hb, emb)
            mine = exchange_stats(st, tgt_loc.reshape(1, n).astype(jnp.float32), n_tp, vocab, inv_n)
            plane = jnp.stack([mine] + [over(hop, mine) for hop in HOPS[1:]])
            dhg = backward_h(lg, emb, mine, inv, hid, res, inv_n)
            dhg = lax.psum(dhg, 'tp')
            sums = jnp.concatenate([jnp.sum(dhg[n:n + 8], axis=0), jnp.full((n,), jnp.sum(dhg[n + 8:]) * inv_n)]).reshape(3 * n // 128, 128)
            for hop in "cxy":
                back = over(hop, sums)
                sums = sums + back
            sums = sums.reshape(3 * n)
            grad_w, loss = sums[:d], sums[2 * n]
            order = jnp.stack([flipped(dp, hop) for hop in HOPS])

            f0 = n_dp * RA
            fh = NF * R
            core = dp % 2
            off = (f0 + core * fh + R * jnp.arange(NF)).astype(jnp.int32)
            gate = lax.optimization_barrier
            a, hs = plane_rows(emb, plane, [s1, s2, x1, x2, y1, y2], 2, inv_n, 1, lambda i: lax.rem(i + 6, 7), own=(lg, hb))
            acc = chip_rows(off, lg, emb, plane, hb, hs, 6, NF, inv_n)
            a, _ = gate((a, acc))
            a1, a2, hs = plane_rows(emb, plane, [d1, d2], 1, inv_n, 2, lambda i: i + 4, acc=a, so_far=hs)
            ax1, ay2 = over_x(a1), over_y(a2)
            ax2, ay1 = over_x(a2), over_y(a1)
            as1, as2 = over_c(a1), over_c(a2)
            ad1, ad2 = over_y(ax1), over_x(ay2)
            axs1, ays2 = over_c(ax1), over_c(ay2)
            axs2, ays1 = over_c(ax2), over_c(ay1)
            ads1, ads2 = over_c(ad1), over_c(ad2)
            pieces, last, j = [], a1, 0
            for k, (p1, p2) in enumerate([(a1, a2), (as1, as2), (ax1, ax2), (ay1, ay2), (axs1, axs2), (ays1, ays2), (ad1, ad2), (ads1, ads2)]):
                pieces += [(p1, 1 + k, 0), (p2, 1 + k, RA // 2)]
            tail = vocab - f0 - fh
            grad_emb = None
            for cnt in GROUPS:
                acc, last = gate((acc, last))
                last, grad_emb = rest_rows(off, j, cnt, 3, emb, plane, acc, hs, inv_n, grad_emb)
                other = over_c(last)
                pieces = [(other, LAST, j * R)] + pieces
                if j * R <= tail < (j + cnt) * R:
                    ending = (last, other, tail // 8 * 8 - j * R)
                j += cnt
            pos = jnp.concatenate([jnp.stack([f0 + fh]), order * RA, jnp.stack([f0 + core * fh, f0 + (1 - core) * fh])]).astype(jnp.int32)

            def of(*arrays):
                return [p for p in pieces if any(p[0] is q for q in arrays)]

            early = [p for p in pieces if all(p[0] is not q for q in (axs2, ays1, ad1, ad2, ads1, ads2, other))]
            grad_emb = place(pos, early, vocab, d, tail, grad_emb)
            grad_r = resid_grad(dhg, hid, res, inv, w)
            grad_emb, grad_r = gate((grad_emb, grad_r))
            grad_emb = place(pos, of(other, axs2, ays1), vocab, d, tail, grad_emb)
            grad_emb = place(pos, of(ad1, ad2), vocab, d, tail, grad_emb)
            grad_emb = place(pos, of(ads1, ads2), vocab, d, tail, grad_emb)
            if vocab % 8:
                grad_emb = place_tail(pos, *ending, grad_emb)
            return loss, grad_r.reshape(hid_loc.shape), grad_emb, grad_w

        sharded = jax.shard_map(
            body, mesh=mesh,
            in_specs=(P('dp', None, None), P('dp', None, None), P('dp', None), P('tp', None), P(None)),
            out_specs=(P(), P('dp', None, None), P('tp', None), P(None)),
            check_vma=False)
        return sharded(hidden, residual, targets, embedding, norm_w)

    return program
```
